32 devices in a mesh: owner: 4 (over y, x), rows: 8 (over z, core).
Axes of the slice: x: 2, y: 2, z: 4, core: 2. Of those that a mesh axis runs over, the one named last changes fastest.
Arguments:
- train_gate: float32 [64, 2048, 1024], P('owner', 'rows'), may hold values from -0.1875 to 0.1875
- train_up: float32 [64, 2048, 1024], P('owner', 'rows'), may hold values from -0.1875 to 0.1875
- train_down: float32 [64, 1024, 2048], P('owner', None, 'rows'), may hold values from -0.25 to 0.25
- router_weight: float32 [2048, 64], P('rows', 'owner'), may hold values from -0.125 to 0.125
- router_gain: float32 [2048], P('rows'), may hold values from 0.25 to 1.75
Outputs:
- ready_gate: bfloat16 [64, 2048, 1024], P('owner', None, 'rows')
- ready_up: bfloat16 [64, 2048, 1024], P('owner', None, 'rows')
- ready_down: bfloat16 [64, 1024, 2048], P('owner', 'rows')
- scale_gate: float32 [64, 1024], P('owner', 'rows')
- scale_up: float32 [64, 1024], P('owner', 'rows')
- scale_down: float32 [64, 1024], P('owner', 'rows')
- serve_router: bfloat16 [2048, 64], replicated
The draws below stay inside these ranges and needn't reach their ends.
All inputs are finite; a program needn't handle non-finite values. Where the reference program divides by a largest or mean magnitude, that divisor is 1e-20 or more.
Results may differ from the reference program's by a relative error of at most 0.0013.
Values may be sent and summed in bfloat16 or wider, within the bound.
A program may use at most 192 MiB of HBM per device.

```python
import jax
import jax.numpy as jnp

EXPERTS = 64
D_MODEL = 2048
D_EXPERT = 1024


def raised(drawn, own_key, source, target, parts, factor):
    owner, partner = [(jnp.arange(drawn.shape[axis_at]) // (drawn.shape[axis_at] // parts)).reshape([-1 if axis == axis_at else 1 for axis in range(drawn.ndim)]) for axis_at in (source, target)]
    chosen = jax.random.permutation(own_key, parts)[partner]
    strong = (owner == chosen) | (owner == (partner + parts // 2) % parts)
    return jnp.where(strong, factor * drawn, drawn)


def steps_of(rng, dims, shards, low, top_value):
    def one(dim, parts):
        heights = jax.random.uniform(jax.random.fold_in(jax.random.fold_in(rng, 6), dim), (parts,), jnp.float32, low / len(shards), top_value / len(shards))
        return jnp.repeat(jnp.exp(heights), dims[dim] // parts).reshape((-1,) + (1,) * (len(dims) - dim - 1))

    factor_of = one(*shards[0])
    for cut in shards[1:]:
        factor_of = factor_of * one(*cut)
    return factor_of


def bell_draw(own_key, shape, scale, reach, pieces=(), dtype=jnp.bfloat16):
    result = scale * jax.random.normal(own_key, shape, jnp.float32)
    if pieces:
        result = result * steps_of(own_key, shape, pieces, -0.22, 0.18)
    return jnp.clip(result, -reach, reach).astype(dtype)


def bell_draw_with(own_key, dims, deviation, reach, split, heavy, kind=jnp.bfloat16):
    result = deviation * jax.random.normal(own_key, dims, jnp.float32)
    if split:
        result = result * steps_of(own_key, dims, split, -0.22, 0.18)
    return jnp.clip(raised(result, jax.random.fold_in(own_key, 3), *heavy), -reach, reach).astype(kind)


def setup_inputs(seed: int = 0) -> dict:
    splits = jax.random.split(jax.random.key(seed), 6)
    train_gate = bell_draw_with(splits[0], (EXPERTS, D_MODEL, D_EXPERT), D_MODEL ** -0.5, 0.1875, ((0, 4), (1, 8)), (1, 2, 8, 2.0), jnp.float32)
    train_up = bell_draw_with(splits[1], (EXPERTS, D_MODEL, D_EXPERT), D_MODEL ** -0.5, 0.1875, ((0, 4), (1, 8)), (1, 2, 8, 2.0), jnp.float32)
    train_down = bell_draw_with(splits[2], (EXPERTS, D_EXPERT, D_MODEL), D_EXPERT ** -0.5, 0.25, ((0, 4), (2, 8)), (2, 1, 8, 2.0), jnp.float32)
    router_weight = bell_draw(splits[3], (D_MODEL, EXPERTS), D_MODEL ** -0.5, 0.125, ((0, 8), (1, 4)), jnp.float32)
    router_gain = jnp.clip(1.0 + 0.15 * jax.random.normal(splits[4], (D_MODEL,), jnp.float32), 0.25, 1.75)
    return {"train_gate": train_gate, "train_up": train_up, "train_down": train_down, "router_weight": router_weight, "router_gain": router_gain}


def reference(train_gate, train_up, train_down, router_weight, router_gain):
    scale_gate = jnp.sum(jnp.abs(train_gate), axis=1) / D_MODEL
    ready_gate = (train_gate / jnp.expand_dims(scale_gate, 1)).astype(jnp.bfloat16)
    scale_up = jnp.sum(jnp.abs(train_up), axis=1) / D_MODEL
    ready_up = (train_up / jnp.expand_dims(scale_up, 1)).astype(jnp.bfloat16)
    scale_down = jnp.sum(jnp.abs(train_down), axis=2) / D_MODEL
    ready_down = (train_down / jnp.expand_dims(scale_down, 2)).astype(jnp.bfloat16)
    serve_router = (router_weight * router_gain[:, None]).astype(jnp.bfloat16)
    return ready_gate, ready_up, ready_down, scale_gate, scale_up, scale_down, serve_router
```

```python
import functools

import jax
import jax.numpy as jnp
from jax import lax
from jax.experimental import pallas as pl
from jax.experimental.pallas import tpu as pltpu
from jax.sharding import PartitionSpec as P

CORES = 2
SLOTS = 4
GROUPS = 4
MESH = pl.DeviceIdType.MESH


def exchange(
    n,
    owners,
    gate,
    up,
    down,
    router,
    out_gate,
    out_up,
    out_down,
    out_scale,
    out_router,
    wide,
    tall,
    send_wide,
    send_tall,
    part,
    arrived,
    inverse,
    load_sem,
    own_sem,
    sum_send,
    sum_recv,
    inv_send,
    inv_recv,
    row_send,
    row_recv,
    col_send,
    col_recv,
    send_sem,
    recv_sem,
):
    me = lax.axis_index("rows")
    home = lax.axis_index("owner")
    experts, rows, _ = gate.shape
    share = out_gate.shape[2]
    slots = min(SLOTS, experts)
    per = max(1, experts // GROUPS)
    groups = experts // per
    chips = n // CORES
    chip = me // CORES
    core = lax.rem(me, CORES)

    def peer(k):
        return lax.rem(me + k, n)

    def remote(src, dst, out_sem, in_sem, **where):
        return pltpu.make_async_remote_copy(
            src_ref=src,
            dst_ref=dst,
            send_sem=out_sem,
            recv_sem=in_sem,
            device_id=where,
            device_id_type=MESH,
        )

    barrier = pltpu.get_barrier_semaphore()
    for k in range(1, n):
        pl.semaphore_signal(barrier, inc=1, device_id={"rows": peer(k)}, device_id_type=MESH)
    for k in range(1, owners):
        pl.semaphore_signal(
            barrier, inc=1, device_id={"owner": lax.rem(home + k, owners)}, device_id_type=MESH
        )

    def load(src, buf, e):
        slot = lax.rem(e, slots)
        kind = 0 if buf is wide else 1
        return pltpu.make_async_copy(src.at[e], buf.at[slot], load_sem.at[kind, slot])

    def fill(src, buf):
        for e in range(slots):
            load(src, buf, e).start()

    def take(src, buf, e, body):
        load(src, buf, e).wait()
        body(e, lax.rem(e, slots))

        @pl.when(e + slots < experts)
        def _():
            load(src, buf, e + slots).start()

    def sums_wide(t):
        def body(e, slot):
            for j in range(n):
                block = wide[slot, :, j * share : (j + 1) * share]
                part[j, t, e] = jnp.sum(jnp.abs(block), axis=0, keepdims=True)

        return body

    def sums_tall(e, slot):
        for j in range(n):
            block = tall[slot, j * share : (j + 1) * share, :]
            part[j, 2, e] = jnp.sum(jnp.abs(block).T, axis=0, keepdims=True)

    def run(src, buf, body):
        fill(src, buf)

        @pl.loop(0, experts)
        def _(e):
            take(src, buf, e, body)

    run(gate, wide, sums_wide(0))

    pl.semaphore_wait(barrier, n - 1 + owners - 1)

    stages = (pl.ds(0, 1), pl.ds(1, 2))

    def sum_copy(stage, to, src):
        return remote(
            part.at[to, stages[stage]],
            arrived.at[src, stages[stage]],
            sum_send.at[stage, to],
            sum_recv.at[stage, src],
            rows=to,
        )

    def inv_copy(stage, to, src):
        block = inverse.at[src, stages[stage]]
        return remote(block, block, inv_send.at[stage, to], inv_recv.at[stage, src], rows=to)

    def send_sums(stage):
        for k in range(1, n):
            sum_copy(stage, peer(k), me).start()

    def send_inverse(stage):
        total = part[me, stages[stage]]
        for k in range(1, n):
            sum_copy(stage, peer(k), peer(k)).wait_recv()
            total = total + arrived[peer(k), stages[stage]]
        scale = total / (rows * n)
        out_scale[stages[stage]] = scale
        inverse[me, stages[stage]] = 1.0 / scale
        for k in range(1, n):
            inv_copy(stage, peer(k), me).start()

    def await_inverse(stage):
        for k in range(1, n):
            inv_copy(stage, peer(k), peer(k)).wait_recv()

    def row_copy(to, src):
        return remote(
            router,
            out_router.at[home, :, pl.ds(pl.multiple_of(src * rows, rows), rows)],
            row_send.at[to],
            row_recv.at[src],
            rows=to,
        )

    def col_copy(to, src):
        return remote(
            out_router.at[src], out_router.at[src], col_send.at[to], col_recv.at[src], owner=to
        )

    send_sums(0)
    fill(gate, wide)
    for k in range(1, n):
        row_copy(peer(k), me).start()
    mine = out_router.at[home, :, pl.ds(pl.multiple_of(me * rows, rows), rows)]
    own_router = pltpu.make_async_copy(router, mine, own_sem.at[0])
    own_router.start()
    send_inverse(0)
    await_inverse(0)

    def block_copy(t, g, to, src):
        some = pl.ds(g * per, per)
        span = pl.ds(pl.multiple_of(src * rows, rows), rows)
        if t < 2:
            piece = send_wide.at[t, to, some]
            dst = (out_gate, out_up)[t].at[some, span, :]
        else:
            piece = send_tall.at[to, some]
            dst = out_down.at[some, :, span]
        return remote(piece, dst, send_sem.at[t, g, to], recv_sem.at[t, g, src], rows=to)

    def own_copy(t):
        span = pl.ds(pl.multiple_of(me * rows, rows), rows)
        if t < 2:
            return pltpu.make_async_copy(
                send_wide.at[t, me], (out_gate, out_up)[t].at[:, span, :], own_sem.at[1 + t]
            )
        return pltpu.make_async_copy(send_tall.at[me], out_down.at[:, :, span], own_sem.at[1 + t])

    def send_at(t, g, d):
        for side in (1, -1):
            there = chip + side * d

            @pl.when((there >= 0) & (there < chips))
            def _():
                for c in range(CORES):
                    block_copy(t, g, there * CORES + lax.rem(core + c, CORES), me).start()

    def ready_wide(t):
        def body(e, slot):
            for j in range(n):
                block = wide[slot, :, j * share : (j + 1) * share]
                send_wide[t, j, e] = (block * inverse[j, t, e]).astype(jnp.bfloat16)

        return body

    def ready_tall(e, slot):
        for j in range(n):
            block = tall[slot, j * share : (j + 1) * share, :]
            factor = jnp.broadcast_to(inverse[j, 2, e], (rows, share)).T
            send_tall[j, e] = (block * factor).astype(jnp.bfloat16)

    def send_near(t, g):
        send_at(t, g, 1)
        for c in range(1, CORES):
            block_copy(t, g, chip * CORES + lax.rem(core + c, CORES), me).start()

    def ready(t, src, buf, body, sent):
        @pl.loop(0, groups)
        def _(g):
            @pl.loop(0, per)
            def _(i):
                take(src, buf, g * per + i, body)

            @pl.when(g < sent)
            def _():
                send_near(t, g)

        own_copy(t).start()

    early = max(1, groups - 1)
    ahead = min(2, groups)
    ready(0, gate, wide, ready_wide(0), early)
    run(up, wide, sums_wide(1))
    run(down, tall, sums_tall)
    send_sums(1)
    fill(up, wide)
    fill(down, tall)
    for g in range(early, groups):
        send_near(0, g)
    send_inverse(1)
    if chips > 2:
        for g in range(ahead):
            send_at(0, g, 2)
    await_inverse(1)
    ready(1, up, wide, ready_wide(1), groups)
    ready(2, down, tall, ready_tall, groups)

    for k in range(1, n):
        row_copy(peer(k), peer(k)).wait_recv()
    own_router.wait()
    for k in range(1, owners):
        col_copy(lax.rem(home + k, owners), home).start()

    if chips > 2:

        @pl.loop(ahead, groups)
        def _(g):
            send_at(0, g, 2)

        for t in (1, 2):

            @pl.loop(0, groups)
            def _(g):
                send_at(t, g, 2)

    @pl.loop(3, max(3, chips))
    def _(d):
        for t in range(3):

            @pl.loop(0, groups)
            def _(g):
                send_at(t, g, d)

    for k in range(1, owners):
        other = lax.rem(home + k, owners)
        col_copy(other, other).wait_recv()
        col_copy(other, home).wait_send()
    for k in range(1, n):
        for stage in range(2):
            sum_copy(stage, peer(k), me).wait_send()
            inv_copy(stage, peer(k), me).wait_send()
        row_copy(peer(k), me).wait_send()
    for t in range(3):
        own_copy(t).wait()

        @pl.loop(0, groups)
        def _(g):
            @pl.loop(1, n)
            def _(k):
                block_copy(t, g, peer(k), peer(k)).wait_recv()
                block_copy(t, g, peer(k), me).wait_send()


def local(n, owners, gate, up, down, router_weight, router_gain):
    experts, rows, width = gate.shape
    share = width // n
    per = max(1, experts // GROUPS)
    groups = experts // per
    slots = min(SLOTS, experts)
    router = (router_weight * router_gain[:, None]).T.astype(jnp.bfloat16)
    anywhere = pl.BlockSpec(memory_space=pl.ANY)
    f32, bf16 = jnp.float32, jnp.bfloat16
    dma = pltpu.SemaphoreType.DMA
    ready_gate, ready_up, ready_down, scales, columns = pl.pallas_call(
        functools.partial(exchange, n, owners),
        name="exchange",
        out_shape=(
            jax.ShapeDtypeStruct((experts, rows * n, share), bf16),
            jax.ShapeDtypeStruct((experts, rows * n, share), bf16),
            jax.ShapeDtypeStruct((experts, share, rows * n), bf16),
            jax.ShapeDtypeStruct((3, experts, 1, share), f32),
            jax.ShapeDtypeStruct((owners, router.shape[0], rows * n), bf16),
        ),
        in_specs=[anywhere] * 4,
        out_specs=(
            anywhere,
            anywhere,
            anywhere,
            pl.BlockSpec(memory_space=pltpu.VMEM),
            anywhere,
        ),
        scratch_shapes=[
            pltpu.VMEM((slots, rows, width), f32),
            pltpu.VMEM((slots, width, rows), f32),
            pltpu.VMEM((2, n, experts, rows, share), bf16),
            pltpu.VMEM((n, experts, share, rows), bf16),
            pltpu.VMEM((n, 3, experts, 1, share), f32),
            pltpu.VMEM((n, 3, experts, 1, share), f32),
            pltpu.VMEM((n, 3, experts, 1, share), f32),
            dma((2, slots)),
            dma((4,)),
            dma((2, n)),
            dma((2, n)),
            dma((2, n)),
            dma((2, n)),
            dma((n,)),
            dma((n,)),
            dma((owners,)),
            dma((owners,)),
            dma((3, groups, n)),
            dma((3, groups, n)),
        ],
        compiler_params=pltpu.CompilerParams(
            collective_id=0, has_side_effects=True, vmem_limit_bytes=58 * 1024 * 1024
        ),
    )(gate, up, down, router)
    serve_router = jnp.transpose(columns, (2, 0, 1)).reshape(rows * n, -1)
    scale_gate, scale_up, scale_down = (scales[t].reshape(experts, share) for t in range(3))
    return (ready_gate, ready_up, ready_down, scale_gate, scale_up, scale_down, serve_router)


def solution(mesh):
    return jax.shard_map(
        functools.partial(local, mesh.shape["rows"], mesh.shape["owner"]),
        mesh=mesh,
        in_specs=(
            P("owner", "rows", None),
            P("owner", "rows", None),
            P("owner", None, "rows"),
            P("rows", "owner"),
            P("rows"),
        ),
        out_specs=(
            P("owner", None, "rows"),
            P("owner", None, "rows"),
            P("owner", "rows", None),
            P("owner", "rows"),
            P("owner", "rows"),
            P("owner", "rows"),
            P(),
        ),
        check_vma=False,
    )
```
